32 devices in a mesh: sweep: 4 (over z), layer: 8 (over y, x, core).
Axes of the slice: x: 2, y: 2, z: 4, core: 2. Of those that a mesh axis runs over, the one named last changes fastest.
Arguments:
- green: bfloat16 [4, 2, 8192, 8192], P('sweep', None, 'layer'), may hold values from -1 to 1
- down_source: float32 [4, 2, 16, 8192], P('sweep', None, None, 'layer'), may hold values from -6 to 6
- up_source: float32 [4, 2, 16, 8192], P('sweep', None, None, 'layer'), may hold values from -6 to 6
Outputs:
- total: float32 [4, 2, 16, 8192], P('sweep', None, None, 'layer')
The draws below stay inside these ranges and needn't reach their ends.
All inputs are finite; a program needn't handle non-finite values.
Results may differ from the reference program's by a relative error of at most 0.02.
Values may be sent and summed in bfloat16 or wider, within the bound.
A program may use at most 64 MiB of HBM per device.

```python
import math
import jax
import jax.numpy as jnp
from jax import lax

W = 8192
SOURCES = 16
LAYERS = 4


def draw_green(key, part):
    base_key = jax.random.fold_in(key, 7)
    spread = 0.5 / math.sqrt(2.0 * W)

    def draw_layer(layer_index):
        layer_key = jax.random.fold_in(base_key, layer_index)
        key_offdiag, key_modulus, key_angles = jax.random.split(layer_key, 3)
        offdiag = jax.random.normal(key_offdiag, (2, W, W), jnp.float32) * spread
        modulus = jax.random.uniform(key_modulus, (W,), jnp.float32, 0.6, 0.9)
        angles = jax.random.uniform(key_angles, (W,), jnp.float32, -jnp.pi, jnp.pi)
        diagonal = jnp.stack([modulus * jnp.cos(angles), modulus * jnp.sin(angles)])
        row_ids = lax.broadcasted_iota(jnp.int32, (W, W), 0)
        col_ids = lax.broadcasted_iota(jnp.int32, (W, W), 1)
        on_diagonal = jnp.where(row_ids == col_ids, 1.0, 0.0).astype(jnp.float32)
        matrix = offdiag + on_diagonal[None] * diagonal[:, :, None]
        matrix = jnp.clip(matrix, -1.0, 1.0)
        return matrix.astype(jnp.bfloat16)
    return lax.map(draw_layer, jnp.arange(LAYERS, dtype=jnp.int32))


def steps_of(own_key, shape, cuts, least, high):
    level, own = 1.0, jax.random.fold_in(own_key, 6)
    for axis_at, shards_of in cuts:
        heights = jnp.exp(jax.random.uniform(jax.random.fold_in(own, axis_at), (shards_of,), jnp.float32, least / len(cuts), high / len(cuts)))
        level = level * jnp.repeat(heights, shape[axis_at] // shards_of).reshape([-1 if axis == axis_at else 1 for axis in range(len(shape))])
    return level


def bell_draw(stream_key, shape, deviation, reach, cuts=(), held_as=jnp.bfloat16):
    factor_of = steps_of(stream_key, shape, cuts, -0.22, 0.18) if cuts else 1.0
    array = jax.random.normal(stream_key, shape, jnp.float32) * deviation * factor_of
    return jnp.minimum(jnp.maximum(array, -reach), reach).astype(held_as)


def setup_inputs(seed: int = 0) -> dict:
    streams_of = jax.random.split(jax.random.key(seed), 4)
    green = draw_green(jax.random.fold_in(streams_of[3], 71), 0)
    down_source = bell_draw(streams_of[1], (LAYERS, 2, SOURCES, W), 1.0, 6.0, ((0, 4), (3, 8)), jnp.float32)
    up_source = bell_draw(streams_of[2], (LAYERS, 2, SOURCES, W), 1.0, 6.0, ((0, 4), (3, 8)), jnp.float32)
    return {"green": green, "down_source": down_source, "up_source": up_source}


def rows_product(trace_in, matrix):
    contract = (((1,), (1,)), ((), ()))
    real_real = lax.dot_general(trace_in[0], matrix[0], contract, preferred_element_type=jnp.float32)
    imag_imag = lax.dot_general(trace_in[1], matrix[1], contract, preferred_element_type=jnp.float32)
    real_imag = lax.dot_general(trace_in[0], matrix[1], contract, preferred_element_type=jnp.float32)
    imag_real = lax.dot_general(trace_in[1], matrix[0], contract, preferred_element_type=jnp.float32)
    return jnp.stack([real_real - imag_imag, real_imag + imag_real])


def cols_product(trace_in, matrix):
    real_real = jnp.dot(trace_in[0], matrix[0], preferred_element_type=jnp.float32)
    imag_imag = jnp.dot(trace_in[1], matrix[1], preferred_element_type=jnp.float32)
    real_imag = jnp.dot(trace_in[0], matrix[1], preferred_element_type=jnp.float32)
    imag_real = jnp.dot(trace_in[1], matrix[0], preferred_element_type=jnp.float32)
    return jnp.stack([real_real - imag_imag, real_imag + imag_real])


def reference(green, down_source, up_source):
    layers = green.shape[0]
    outgoing = jnp.zeros((2, SOURCES, W), jnp.bfloat16)
    down_list = []
    for layer_index in range(layers):
        down_row = down_source[layer_index] + rows_product(outgoing, green[layer_index])
        down_list.append(down_row)
        outgoing = down_row.astype(jnp.bfloat16)
    outgoing = jnp.zeros((2, SOURCES, W), jnp.bfloat16)
    total_list = [None] * layers
    for layer_index in reversed(range(layers)):
        total_row = (up_source[layer_index] + down_list[layer_index]) + cols_product(outgoing, green[layer_index])
        total_list[layer_index] = total_row
        outgoing = total_row.astype(jnp.bfloat16)
    return jnp.stack(total_list)
```

```python
import functools

import jax
import jax.numpy as jnp
from jax import lax
from jax.experimental import pallas as pl
from jax.experimental.pallas import tpu as pltpu
from jax.sharding import PartitionSpec as P

MESH = pl.DeviceIdType.MESH
F32, BF16 = jnp.float32, jnp.bfloat16
GROUPS = 4


def turned(trace):
    half = trace.shape[0] // 2
    return jnp.concatenate([-trace[half:], trace[:half]], axis=0)


def dot(trace, block):
    return jnp.dot(trace, block, preferred_element_type=F32)


def sweeps(layers, peers, blocks, green, down_hbm, up_hbm, total,
           matrix, down_src, up_src, gathered, incoming, part_out, part_in, out_down, out_up, base, acc,
           src_sem, load_sem, dsend, drecv, gsend, grecv, usend, urecv, psend, precv):
    z, j = lax.axis_index("sweep"), lax.axis_index("layer")
    own = down_src.shape[1]
    width = own // blocks
    groups = min(GROUPS, peers)
    per = peers // groups
    odd = lax.rem(z, 2) == 1

    def span(k):
        return pl.ds(pl.multiple_of(k * width, width), width)

    def cols(i, k):
        return pl.ds(pl.multiple_of(i * own + k * width, width), width)

    def peer(d):
        i, bit = j, 1
        while bit < peers:
            if d & bit:
                i = i + bit - 2 * bit * lax.rem(j // bit, 2)
            bit *= 2
        return i

    others = range(peers - 1, 0, -1)

    def load(m, part, g):
        at = (part, span(m), pl.ds(g * per * own, per * own))
        return pltpu.make_async_copy(green.at[at], matrix.at[at], load_sem.at[m, part, g])

    def start_loads():
        for m in range(blocks):
            for g in range(groups):
                for part in (0, 1):
                    load(m, part, g).start()

    def wait_load(m):
        for g in range(groups):
            for part in (0, 1):
                load(m, part, g).wait()

    sources = [pltpu.make_async_copy(down_hbm, down_src, src_sem.at[0]),
               pltpu.make_async_copy(up_hbm, up_src, src_sem.at[1])]

    def remote(src, dst, send, recv, to):
        return pltpu.make_async_remote_copy(
            src_ref=src, dst_ref=dst, send_sem=send, recv_sem=recv, device_id=to, device_id_type=MESH)

    def pass_down(k):
        return remote(out_down.at[k], gathered.at[k, j], dsend.at[k], drecv.at[k], {"sweep": z + 1})

    def pass_up(k):
        return remote(out_up.at[k], incoming.at[k], usend.at[k], urecv.at[k], {"sweep": z - 1})

    def relay(k, d):
        return remote(gathered.at[k, j], gathered.at[k, j], gsend.at[k, d], grecv.at[k, j], {"layer": peer(d)})

    def relayed(k, d):
        i = peer(d)
        return remote(gathered.at[k, i], gathered.at[k, i], gsend.at[k, d], grecv.at[k, i], {"layer": i})

    def share(d, k):
        i = peer(d)
        return remote(part_out.at[i, k], part_in.at[j, k], psend.at[d, k], precv.at[j, k], {"layer": i})

    def shared(d, k):
        i = peer(d)
        return remote(part_out.at[i, k], part_in.at[i, k], psend.at[d, k], precv.at[i, k], {"layer": i})

    @pl.when(z > 0)
    def _():
        start_loads()

    for copy in sources:
        copy.start()

    barrier = pltpu.get_barrier_semaphore()
    for d in others:
        pl.semaphore_signal(barrier, inc=1, device_id={"layer": peer(d)}, device_id_type=MESH)
    for step in (1, layers - 1):
        pl.semaphore_signal(barrier, inc=1, device_id={"sweep": lax.rem(z + step, layers)}, device_id_type=MESH)

    def take(k):
        remote(out_down.at[k], gathered.at[k, j], dsend.at[k], drecv.at[k], {"sweep": z}).wait_recv()
        for d in others:
            relay(k, d).start()

    def flip(m, g):
        for part in (0, 1):
            load(m, part, g).wait()
        for i in range(g * per, (g + 1) * per):
            for k in range(blocks):
                for part in (0, 1):
                    at = (part, span(m), cols(i, k))
                    matrix[at] = matrix[at].T

    @pl.when(z > 0)
    def _():
        for g in range(groups):
            flip(0, g)

    pl.semaphore_wait(barrier, peers + 1)

    def finish_down(k, value, last):
        sum_of = up_src[:, span(k)] + value

        def go_on():
            base[:, span(k)] = sum_of
            out_down[k] = value.astype(BF16)
            pass_down(k).start()

        def turn_back():
            total[:, span(k)] = sum_of
            out_up[k] = sum_of.astype(BF16)
            pass_up(k).start()

        if last is None:
            pl.when(z < layers - 1)(go_on)
            pl.when(z == layers - 1)(turn_back)
        elif last:
            turn_back()
        else:
            go_on()

    even_last = None if layers % 2 else False
    odd_last = True if layers == 4 else None

    def wait_gather(k):
        for d in others:
            relayed(k, d).wait_recv()

    def down_term(m, ks):
        value = None
        for k in ks:
            for i in range(peers):
                trace = gathered[k, i]
                term = dot(trace, matrix[0, span(m), cols(i, k)])
                value = term if value is None else value + term
                value = value + dot(turned(trace), matrix[1, span(m), cols(i, k)])
        return value

    def again():
        @pl.when(z < layers - 1)
        def _():
            start_loads()

    def wait_sources():
        for copy in sources:
            copy.wait()

    @pl.when(z == 0)
    def _():
        wait_sources()

        @pl.loop(0, blocks)
        def _(k):
            finish_down(k, down_src[:, span(k)], False)

        start_loads()

    @pl.when(z > 0)
    def _():
        @pl.loop(1, blocks)
        def _(m):
            for g in range(groups):
                flip(m, g)
                if g == 0:
                    @pl.when((z == 1) & (m == blocks // 2))
                    def _():
                        @pl.loop(0, blocks)
                        def _(k):
                            take(k)
        wait_sources()

    @pl.when(z == 1)
    def _():
        @pl.loop(0, blocks)
        def _(k):
            wait_gather(k)

        @pl.loop(0, blocks)
        def _(m):
            finish_down(m, down_src[:, span(m)] + down_term(m, range(blocks)), False)

        again()

    @pl.when(odd & (z > 1))
    def _():
        early = blocks // 2
        base[...] = down_src[...]

        @pl.loop(0, blocks)
        def _(k):
            take(k)

        @pl.loop(0, early)
        def _(k):
            wait_gather(k)
            for m in range(blocks):
                base[:, span(m)] += down_term(m, [k])

        @pl.loop(early, blocks)
        def _(k):
            wait_gather(k)

        @pl.loop(0, blocks)
        def _(m):
            finish_down(m, base[:, span(m)] + down_term(m, range(early, blocks)), odd_last)

        again()

    @pl.when(jnp.logical_not(odd) & (z > 0))
    def _():
        base[...] = down_src[...]
        take(0)

        @pl.loop(0, blocks - 1)
        def _(k):
            take(k + 1)
            wait_gather(k)
            for m in range(blocks):
                base[:, span(m)] += down_term(m, [k])

        wait_gather(blocks - 1)
        for m in range(blocks):
            finish_down(m, base[:, span(m)] + down_term(m, [blocks - 1]), even_last)

        again()

    def wait_up(k):
        remote(out_up.at[k], incoming.at[k], usend.at[k], urecv.at[k], {"sweep": z}).wait_recv()

    def up_term(i, k, rs):
        value = None
        for r in rs:
            trace = incoming[r]
            term = dot(trace, matrix[0, span(r), cols(i, k)])
            value = term if value is None else value + term
            value = value + dot(turned(trace), matrix[1, span(r), cols(i, k)])
        return value

    def finish_up(k):
        value = acc[j, :, span(k)]
        for d in range(1, peers):
            value = value + part_in[peer(d), k].astype(F32)
        value = base[:, span(k)] + value
        total[:, span(k)] = value

        @pl.when(z > 0)
        def _():
            out_up[k] = value.astype(BF16)
            pass_up(k).start()

    def up(early):
        acc[...] = jnp.zeros_like(acc)

        @pl.loop(0, early)
        def _(r):
            wait_load(r)
            wait_up(r)
            for i in range(peers):
                for k in range(blocks):
                    acc[i, :, span(k)] += up_term(i, k, [r])

        @pl.loop(early, blocks)
        def _(r):
            wait_load(r)
            wait_up(r)

        late = range(early, blocks)

        @pl.loop(0, blocks)
        def _(k):
            for d in others:
                i = peer(d)
                part_out[i, k] = (acc[i, :, span(k)] + up_term(i, k, late)).astype(BF16)
            for d in others:
                share(d, k).start()

        for k in range(blocks):
            acc[j, :, span(k)] += up_term(j, k, late)

        @pl.loop(0, blocks)
        def _(k):
            for d in others:
                shared(d, k).wait_recv()
            finish_up(k)

        @pl.loop(0, blocks)
        def _(k):
            for d in others:
                share(d, k).wait_send()

    @pl.when(odd & (z < layers - 1))
    def _():
        up(blocks // 2)

    @pl.when(jnp.logical_not(odd) & (z < layers - 1))
    def _():
        up(blocks - 1)

    @pl.when(z < layers - 1)
    def _():
        @pl.loop(0, blocks)
        def _(k):
            pass_down(k).wait_send()

    @pl.when(z > 0)
    def _():
        @pl.loop(0, blocks)
        def _(k):
            pass_up(k).wait_send()
            for d in others:
                relay(k, d).wait_send()


def local(layers, peers, green, down_source, up_source):
    _one, parts, own, wide = green.shape
    sources = down_source.shape[2]
    both = parts * sources
    width = next(w for w in (256, 128) if own % w == 0)
    blocks = own // width
    groups = min(GROUPS, peers)
    vmem = pl.BlockSpec(memory_space=pltpu.VMEM)
    dma = pltpu.SemaphoreType.DMA
    result = pl.pallas_call(
        functools.partial(sweeps, layers, peers, blocks),
        out_shape=pltpu.VMEM((both, own), F32),
        in_specs=[pl.BlockSpec(memory_space=pltpu.HBM)] * 3,
        out_specs=vmem,
        scratch_shapes=[
            pltpu.VMEM((parts, own, wide), BF16),
            pltpu.VMEM((both, own), F32),
            pltpu.VMEM((both, own), F32),
            pltpu.VMEM((blocks, peers, both, width), BF16),
            pltpu.VMEM((blocks, both, width), BF16),
            pltpu.VMEM((peers, blocks, both, width), BF16),
            pltpu.VMEM((peers, blocks, both, width), BF16),
            pltpu.VMEM((blocks, both, width), BF16),
            pltpu.VMEM((blocks, both, width), BF16),
            pltpu.VMEM((both, own), F32),
            pltpu.VMEM((peers, both, own), F32),
            dma((2,)),
            dma((blocks, 2, groups)),
            dma((blocks,)), dma((blocks,)),
            dma((blocks, peers)), dma((blocks, peers)),
            dma((blocks,)), dma((blocks,)),
            dma((peers, blocks)), dma((peers, blocks)),
        ],
        compiler_params=pltpu.CompilerParams(
            collective_id=0, has_side_effects=True, vmem_limit_bytes=60 * 1024 * 1024),
    )(green[0], down_source.reshape(both, own), up_source.reshape(both, own))
    return result.reshape(1, parts, sources, own)


def solution(mesh):
    in_specs = (
        P("sweep", None, "layer", None),
        P("sweep", None, None, "layer"),
        P("sweep", None, None, "layer"),
    )
    out_specs = P("sweep", None, None, "layer")
    body = functools.partial(local, mesh.shape["sweep"], mesh.shape["layer"])
    return jax.shard_map(body, mesh=mesh, in_specs=in_specs, out_specs=out_specs, check_vma=False)
```

```python
import functools

import jax
import jax.numpy as jnp
from jax import lax
from jax.experimental import pallas as pl
from jax.experimental.pallas import tpu as pltpu
from jax.sharding import PartitionSpec as P

MESH = pl.DeviceIdType.MESH
F32, BF16 = jnp.float32, jnp.bfloat16
GROUPS = 4
EARLY = 1


def turned(trace):
    half = trace.shape[0] // 2
    return jnp.concatenate([-trace[half:], trace[:half]], axis=0)


def dot(trace, block):
    return jnp.dot(trace, block, preferred_element_type=F32)


def sweeps(layers, peers, blocks, green, down_hbm, up_hbm, total,
           matrix, down_src, up_src, gathered, incoming, pair_out, pair_in, part_out, part_in, out_down, out_up, base, acc,
           src_sem, load_sem, dsend, drecv, gsend, grecv, fsend, usend, urecv, xsend, xrecv, psend, precv):
    z, j = lax.axis_index("sweep"), lax.axis_index("layer")
    own = down_src.shape[1]
    width = own // blocks
    groups = min(GROUPS, peers)
    per = peers // groups
    odd = lax.rem(z, 2) == 1

    def span(k):
        return pl.ds(pl.multiple_of(k * width, width), width)

    def cols(i, k):
        return pl.ds(pl.multiple_of(i * own + k * width, width), width)

    def peer(d):
        i, bit = j, 1
        while bit < peers:
            if d & bit:
                i = i + bit - 2 * bit * lax.rem(j // bit, 2)
            bit *= 2
        return i

    others = range(peers - 1, 0, -1)
    far = [d for d in others if bin(d // 2).count("1") > 1]
    near = [d for d in others if d not in far]
    halves = range(peers // 2 - 1, 0, -1)

    def load(m, g):
        at = (slice(None), span(m), pl.ds(g * per * own, per * own))
        return pltpu.make_async_copy(green.at[at], matrix.at[at], load_sem.at[m, g])

    def start_loads():
        for m in range(blocks):
            for g in range(groups):
                load(m, g).start()

    def wait_load(m):
        for g in range(groups):
            load(m, g).wait()

    sources = [pltpu.make_async_copy(down_hbm, down_src, src_sem.at[0]),
               pltpu.make_async_copy(up_hbm, up_src, src_sem.at[1])]

    def remote(src, dst, send, recv, to):
        return pltpu.make_async_remote_copy(
            src_ref=src, dst_ref=dst, send_sem=send, recv_sem=recv, device_id=to, device_id_type=MESH)

    def pass_down(k):
        return remote(out_down.at[k], gathered.at[k, j], dsend, drecv.at[k], {"sweep": z + 1})

    def pass_far(k, d):
        return remote(out_down.at[k], gathered.at[k, j], fsend, grecv.at[k],
                      {"sweep": z + 1, "layer": peer(d)})

    def pass_up(k):
        return remote(out_up.at[k], incoming.at[k], usend, urecv.at[k], {"sweep": z - 1})

    def relay(k, d):
        return remote(gathered.at[k, j], gathered.at[k, j], gsend, grecv.at[k], {"layer": peer(d)})

    def swap(k):
        return remote(pair_out.at[k], pair_in.at[k], xsend, xrecv.at[k], {"layer": peer(1)})

    def share(h, k):
        return remote(part_out.at[k, h], part_in.at[k, h], psend, precv.at[k], {"layer": peer(2 * h)})

    @pl.when(z > 0)
    def _():
        start_loads()

    for copy in sources:
        copy.start()

    barrier = pltpu.get_barrier_semaphore()
    def sent(sources_of, sem):
        remote(sources_of, sources_of, sem, sem, {"sweep": z}).wait_send()

    def greet(to):
        pl.semaphore_signal(barrier, inc=1, device_id=to, device_id_type=MESH)

    @pl.when(z > 0)
    def _():
        greet({"sweep": z - 1})
        for d in far:
            greet({"sweep": z - 1, "layer": peer(d)})
        for d in others:
            greet({"layer": peer(d)})

    def take(k):
        remote(out_down.at[k], gathered.at[k, j], dsend, drecv.at[k], {"sweep": z}).wait_recv()
        for d in near:
            relay(k, d).start()

    def flip(m, g):
        load(m, g).wait()
        for i in range(g * per, (g + 1) * per):
            for k in range(blocks):
                for part in (0, 1):
                    at = (part, span(m), cols(i, k))
                    matrix[at] = matrix[at].T

    @pl.when(z > 0)
    def _():
        for g in range(groups):
            flip(0, g)

    @pl.when(z == 0)
    def _():
        pl.semaphore_wait(barrier, 1 + len(far))

    @pl.when((z > 0) & (z < layers - 1))
    def _():
        pl.semaphore_wait(barrier, peers + len(far))

    @pl.when(z == layers - 1)
    def _():
        pl.semaphore_wait(barrier, peers - 1)

    def finish_down(k, value, last):
        sum_of = up_src[:, span(k)] + value

        def go_on():
            base[:, span(k)] = sum_of
            out_down[k] = value.astype(BF16)
            for d in far:
                pass_far(k, d).start()
            pass_down(k).start()

        def turn_back():
            total[:, span(k)] = sum_of
            out_up[k] = sum_of.astype(BF16)
            pass_up(k).start()

        if last is None:
            pl.when(z < layers - 1)(go_on)
            pl.when(z == layers - 1)(turn_back)
        elif last:
            turn_back()
        else:
            go_on()

    even_last = None if layers % 2 else False
    odd_last = True if layers == 4 else None

    def wait_gather(k):
        rest = gathered.at[k, pl.ds(0, peers - 1)]
        remote(rest, rest, gsend, grecv.at[k], {"sweep": z}).wait_recv()

    def down_term(m, ks):
        value = None
        for k in ks:
            for i in range(peers):
                trace = gathered[k, i]
                term = dot(trace, matrix[0, span(m), cols(i, k)])
                value = term if value is None else value + term
                value = value + dot(turned(trace), matrix[1, span(m), cols(i, k)])
        return value

    def again():
        @pl.when(z < layers - 1)
        def _():
            start_loads()

    def wait_sources():
        for copy in sources:
            copy.wait()

    @pl.when(z == 0)
    def _():
        wait_sources()

        @pl.loop(0, blocks)
        def _(k):
            finish_down(k, down_src[:, span(k)], False)

        start_loads()

    @pl.when(z > 0)
    def _():
        @pl.loop(1, blocks)
        def _(m):
            for g in range(groups):
                flip(m, g)
                if g % 2 == 1:
                    @pl.when((z == 1) & (m == blocks // 2))
                    def _():
                        @pl.loop(g // 2 * blocks // 2, (g // 2 + 1) * blocks // 2)
                        def _(k):
                            take(k)
        wait_sources()

    @pl.when(z == 1)
    def _():
        @pl.loop(0, blocks)
        def _(k):
            wait_gather(k)

        @pl.loop(0, blocks)
        def _(m):
            finish_down(m, down_src[:, span(m)] + down_term(m, range(blocks)), False)

        again()

    @pl.when(odd & (z > 1))
    def _():
        early = EARLY
        base[...] = down_src[...]

        @pl.loop(0, blocks)
        def _(k):
            take(k)

        @pl.loop(0, early)
        def _(k):
            wait_gather(k)
            for m in range(blocks):
                base[:, span(m)] += down_term(m, [k])

        @pl.loop(early, blocks)
        def _(k):
            wait_gather(k)

        @pl.loop(0, blocks)
        def _(m):
            finish_down(m, base[:, span(m)] + down_term(m, range(early, blocks)), odd_last)

        again()

    @pl.when(jnp.logical_not(odd) & (z > 0))
    def _():
        base[...] = down_src[...]
        for k in range(min(2, blocks)):
            take(k)

        @pl.loop(0, blocks - 1)
        def _(k):
            wait_gather(k)

            @pl.when(k + 2 < blocks)
            def _():
                take(k + 2)

            for m in range(blocks):
                base[:, span(m)] += down_term(m, [k])

        wait_gather(blocks - 1)
        for m in range(blocks):
            finish_down(m, base[:, span(m)] + down_term(m, [blocks - 1]), even_last)

        again()

    def wait_up(k):
        remote(out_up.at[k], incoming.at[k], usend, urecv.at[k], {"sweep": z}).wait_recv()

    def up_term(i, k, rs):
        value = None
        for r in rs:
            trace = incoming[r]
            term = dot(trace, matrix[0, span(r), cols(i, k)])
            value = term if value is None else value + term
            value = value + dot(turned(trace), matrix[1, span(r), cols(i, k)])
        return value

    def finish_up(k):
        value = acc[j, :, span(k)]
        for h in halves:
            value = value + part_in[k, h].astype(F32)
        value = base[:, span(k)] + value
        total[:, span(k)] = value

        @pl.when(z > 0)
        def _():
            out_up[k] = value.astype(BF16)
            pass_up(k).start()

    def combine(k):
        swap(k).wait_recv()
        for h in halves:
            i = peer(2 * h)
            part_out[k, h] = (acc[i, :, span(k)] + pair_in[k, h].astype(F32)).astype(BF16)
        for h in halves:
            share(h, k).start()
        acc[j, :, span(k)] += pair_in[k, 0].astype(F32)

    def up(early, step):
        acc[...] = jnp.zeros_like(acc)

        @pl.loop(0, early)
        def _(r):
            wait_load(r)
            wait_up(r)
            for i in range(peers):
                for k in range(blocks):
                    acc[i, :, span(k)] += up_term(i, k, [r])

        @pl.loop(early, blocks)
        def _(r):
            wait_load(r)
            wait_up(r)

        late = range(early, blocks)

        def hand_over(k):
            for d in range(peers - 1, 0, -2):
                i = peer(d)
                pair_out[k, d // 2] = (acc[i, :, span(k)] + up_term(i, k, late)).astype(BF16)

        def keep(k):
            for d in range(peers - 2, -1, -2):
                i = peer(d)
                acc[i, :, span(k)] += up_term(i, k, late)

        @pl.loop(0, blocks // step)
        def _(c):
            for n in range(step):
                hand_over(c * step + n)
            for n in range(step):
                swap(c * step + n).start()

        @pl.loop(0, blocks // step)
        def _(c):
            for n in range(step):
                keep(c * step + n)
            for n in range(step):
                combine(c * step + n)

        @pl.loop(0, blocks)
        def _(k):
            shares = pl.ds(0, len(halves))
            remote(part_out.at[k, shares], part_in.at[k, shares], psend, precv.at[k], {"sweep": z}).wait_recv()
            finish_up(k)

        sent(pair_out, xsend)
        sent(part_out.at[:, pl.ds(0, len(halves))], psend)

    @pl.when(odd & (z < layers - 1))
    def _():
        up(blocks // 2, 1)

    @pl.when(jnp.logical_not(odd) & (z < layers - 1))
    def _():
        up(blocks - 1, 2)

    @pl.when(z < layers - 1)
    def _():
        sent(out_down, dsend)
        if far:
            sent(gathered.at[:, pl.ds(0, len(far))], fsend)

    @pl.when(z > 0)
    def _():
        sent(out_up, usend)
        sent(gathered.at[:, pl.ds(0, len(near))], gsend)


def local(layers, peers, green, down_source, up_source):
    _one, parts, own, wide = green.shape
    sources = down_source.shape[2]
    both = parts * sources
    width = next(w for w in (256, 128) if own % w == 0)
    blocks = own // width
    groups = min(GROUPS, peers)
    vmem = pl.BlockSpec(memory_space=pltpu.VMEM)
    dma = pltpu.SemaphoreType.DMA
    result = pl.pallas_call(
        functools.partial(sweeps, layers, peers, blocks),
        out_shape=pltpu.VMEM((both, own), F32),
        in_specs=[pl.BlockSpec(memory_space=pltpu.HBM)] * 3,
        out_specs=vmem,
        scratch_shapes=[
            pltpu.VMEM((parts, own, wide), BF16),
            pltpu.VMEM((both, own), F32),
            pltpu.VMEM((both, own), F32),
            pltpu.VMEM((blocks, peers, both, width), BF16),
            pltpu.VMEM((blocks, both, width), BF16),
            pltpu.VMEM((blocks, peers // 2, both, width), BF16),
            pltpu.VMEM((blocks, peers // 2, both, width), BF16),
            pltpu.VMEM((blocks, peers // 2, both, width), BF16),
            pltpu.VMEM((blocks, peers // 2, both, width), BF16),
            pltpu.VMEM((blocks, both, width), BF16),
            pltpu.VMEM((blocks, both, width), BF16),
            pltpu.VMEM((both, own), F32),
            pltpu.VMEM((peers, both, own), F32),
            dma((2,)),
            dma((blocks, groups)),
            dma(()), dma((blocks,)),
            dma(()), dma((blocks,)),
            dma(()),
            dma(()), dma((blocks,)),
            dma(()), dma((blocks,)),
            dma(()), dma((blocks,)),
        ],
        compiler_params=pltpu.CompilerParams(
            collective_id=0, has_side_effects=True, vmem_limit_bytes=60 * 1024 * 1024),
    )(green[0], down_source.reshape(both, own), up_source.reshape(both, own))
    return result.reshape(1, parts, sources, own)


def solution(mesh):
    in_specs = (
        P("sweep", None, "layer", None),
        P("sweep", None, None, "layer"),
        P("sweep", None, None, "layer"),
    )
    out_specs = P("sweep", None, None, "layer")
    body = functools.partial(local, mesh.shape["sweep"], mesh.shape["layer"])
    return jax.shard_map(body, mesh=mesh, in_specs=in_specs, out_specs=out_specs, check_vma=False)
```

```python
import functools

import jax
import jax.numpy as jnp
from jax import lax
from jax.experimental import pallas as pl
from jax.experimental.pallas import tpu as pltpu
from jax.sharding import PartitionSpec as P

MESH = pl.DeviceIdType.MESH
F32, BF16 = jnp.float32, jnp.bfloat16
GROUPS = 4
EARLY = 3
AHEAD = 1


def turned(trace):
    half = trace.shape[0] // 2
    return jnp.concatenate([-trace[half:], trace[:half]], axis=0)


def dot(trace, block):
    return jnp.dot(trace, block, preferred_element_type=F32)


def sweeps(layers, peers, blocks, green, down_hbm, up_hbm, total,
           matrix, down_src, up_src, gathered, incoming, pair_out, pair_in, part_out, part_in, out_down, out_up, base, acc,
           src_sem, load_sem, dsend, drecv, gsend, grecv, fsend, frecv, usend, urecv, xsend, xrecv, psend, precv):
    z, j = lax.axis_index("sweep"), lax.axis_index("layer")
    own = down_src.shape[1]
    width = own // blocks
    groups = min(GROUPS, peers)
    per = peers // groups
    odd = lax.rem(z, 2) == 1

    def span(k):
        return pl.ds(pl.multiple_of(k * width, width), width)

    def cols(i, k):
        return pl.ds(pl.multiple_of(i * own + k * width, width), width)

    def peer(d):
        i, bit = j, 1
        while bit < peers:
            if d & bit:
                i = i + bit - 2 * bit * lax.rem(j // bit, 2)
            bit *= 2
        return i

    others = range(peers - 1, 0, -1)
    far = [d for d in others if bin(d // 2).count("1") > 1]
    near = [d for d in others if d not in far]
    soon, later = [0, 1] + far, [d for d in near if d > 1]
    halves = range(peers // 2 - 1, 0, -1)

    def load(m, g):
        at = (slice(None), span(m), pl.ds(g * per * own, per * own))
        return pltpu.make_async_copy(green.at[at], matrix.at[at], load_sem.at[m, g])

    def start_loads():
        for m in range(blocks):
            for g in range(groups):
                load(m, g).start()

    def wait_load(m):
        for g in range(groups):
            load(m, g).wait()

    sources = [pltpu.make_async_copy(down_hbm, down_src, src_sem.at[0]),
               pltpu.make_async_copy(up_hbm, up_src, src_sem.at[1])]

    def remote(src, dst, send, recv, to):
        return pltpu.make_async_remote_copy(
            src_ref=src, dst_ref=dst, send_sem=send, recv_sem=recv, device_id=to, device_id_type=MESH)

    def pass_down(k):
        return remote(out_down.at[k], gathered.at[k, j], dsend, drecv.at[k], {"sweep": z + 1})

    def pass_far(k, d):
        return remote(out_down.at[k], gathered.at[k, j], fsend, frecv.at[k],
                      {"sweep": z + 1, "layer": peer(d)})

    def pass_up(k):
        return remote(out_up.at[k], incoming.at[k], usend, urecv.at[k], {"sweep": z - 1})

    def relay(k, d):
        return remote(gathered.at[k, j], gathered.at[k, j], gsend, (frecv if d == 1 else grecv).at[k],
                      {"layer": peer(d)})

    def swap(k):
        return remote(pair_out.at[k], pair_in.at[k], xsend, xrecv.at[k], {"layer": peer(1)})

    def share(h, k):
        return remote(part_out.at[k, h], part_in.at[k, h], psend, precv.at[k], {"layer": peer(2 * h)})

    @pl.when(z > 0)
    def _():
        start_loads()

    for copy in sources:
        copy.start()

    barrier = pltpu.get_barrier_semaphore()
    def sent(sources_of, sem):
        remote(sources_of, sources_of, sem, sem, {"sweep": z}).wait_send()

    def greet(to):
        pl.semaphore_signal(barrier, inc=1, device_id=to, device_id_type=MESH)

    @pl.when(z > 0)
    def _():
        greet({"sweep": z - 1})
        for d in far:
            greet({"sweep": z - 1, "layer": peer(d)})
        for d in others:
            greet({"layer": peer(d)})

    def take(k):
        remote(out_down.at[k], gathered.at[k, j], dsend, drecv.at[k], {"sweep": z}).wait_recv()
        for d in near:
            relay(k, d).start()

    def flip(m, g):
        load(m, g).wait()
        for i in range(g * per, (g + 1) * per):
            for k in range(blocks):
                for part in (0, 1):
                    at = (part, span(m), cols(i, k))
                    matrix[at] = matrix[at].T

    @pl.when(z > 0)
    def _():
        for g in range(groups):
            flip(0, g)

    @pl.when(z == 0)
    def _():
        pl.semaphore_wait(barrier, 1 + len(far))

    @pl.when((z > 0) & (z < layers - 1))
    def _():
        pl.semaphore_wait(barrier, peers + len(far))

    @pl.when(z == layers - 1)
    def _():
        pl.semaphore_wait(barrier, peers - 1)

    def finish_down(k, value, last):
        sum_of = up_src[:, span(k)] + value

        def go_on():
            base[:, span(k)] = sum_of
            out_down[k] = value.astype(BF16)
            for d in far:
                pass_far(k, d).start()
            pass_down(k).start()

        def turn_back():
            total[:, span(k)] = sum_of
            out_up[k] = sum_of.astype(BF16)
            pass_up(k).start()

        if last is None:
            pl.when(z < layers - 1)(go_on)
            pl.when(z == layers - 1)(turn_back)
        elif last:
            turn_back()
        else:
            go_on()

    even_last = None if layers % 2 else False
    odd_last = True if layers == 4 else None

    def wait_some(k, count, sem):
        if count:
            some = gathered.at[k, pl.ds(0, count)]
            remote(some, some, gsend, sem.at[k], {"sweep": z}).wait_recv()

    def wait_soon(k):
        wait_some(k, len(soon) - 1, frecv)

    def wait_later(k):
        wait_some(k, len(later), grecv)

    def wait_gather(k):
        wait_soon(k)
        wait_later(k)

    def down_term(m, pairs):
        value = jnp.zeros((down_src.shape[0], width), F32) if not pairs else None
        for k, ds in pairs:
            for i in (range(peers) if ds is None else map(peer, ds)):
                trace = gathered[k, i]
                term = dot(trace, matrix[0, span(m), cols(i, k)])
                value = term if value is None else value + term
                value = value + dot(turned(trace), matrix[1, span(m), cols(i, k)])
        return value

    def again():
        @pl.when(z < layers - 1)
        def _():
            start_loads()

    def wait_sources():
        for copy in sources:
            copy.wait()

    @pl.when(z == 0)
    def _():
        wait_sources()

        @pl.loop(0, blocks)
        def _(k):
            finish_down(k, down_src[:, span(k)], False)

        start_loads()

    @pl.when(z > 0)
    def _():
        @pl.loop(1, blocks)
        def _(m):
            for g in range(groups):
                flip(m, g)
                if g % 2 == 0:
                    @pl.when((z == 1) & (m == blocks // 2))
                    def _():
                        @pl.loop(g // 2 * blocks // 2, (g // 2 + 1) * blocks // 2)
                        def _(k):
                            take(k)
        wait_sources()

    @pl.when(z == 1)
    def _():
        @pl.loop(0, blocks)
        def _(k):
            wait_gather(k)

        @pl.loop(0, blocks)
        def _(m):
            finish_down(m, down_src[:, span(m)] + down_term(m, [(k, None) for k in range(blocks)]), False)

        again()

    @pl.when(odd & (z > 1))
    def _():
        early = min(EARLY, blocks)
        base[...] = down_src[...]

        @pl.loop(0, blocks)
        def _(k):
            take(k)

        @pl.loop(0, early)
        def _(k):
            wait_soon(k)
            for m in range(blocks):
                base[:, span(m)] += down_term(m, [(k, soon)])

        @pl.loop(early, blocks)
        def _(k):
            wait_soon(k)

        @pl.loop(0, blocks)
        def _(k):
            wait_later(k)

        left = [(k, later) for k in range(early)] + [(k, soon + later) for k in range(early, blocks)]

        @pl.loop(0, blocks)
        def _(m):
            finish_down(m, base[:, span(m)] + down_term(m, left), odd_last)

        again()

    @pl.when(jnp.logical_not(odd) & (z > 0))
    def _():
        base[...] = down_src[...]
        take(0)
        wait_soon(0)
        if blocks > 1:
            take(1)

        @pl.loop(0, blocks - 1)
        def _(k):
            @pl.when(k > 0)
            def _():
                wait_soon(k)

            for m in range(blocks):
                base[:, span(m)] += down_term(m, [(k, soon)])

            @pl.when(k + 2 < blocks)
            def _():
                take(k + 2)

            wait_later(k)
            for m in range(blocks):
                base[:, span(m)] += down_term(m, [(k, later)])

        last = blocks - 1
        if last:
            wait_soon(last)
        for m in range(blocks):
            base[:, span(m)] += down_term(m, [(last, soon)])
        wait_later(last)
        for m in range(blocks):
            finish_down(m, base[:, span(m)] + down_term(m, [(last, later)]), even_last)

        again()

    def wait_up(k):
        remote(out_up.at[k], incoming.at[k], usend, urecv.at[k], {"sweep": z}).wait_recv()

    def up_term(i, k, rs):
        value = None
        for r in rs:
            trace = incoming[r]
            term = dot(trace, matrix[0, span(r), cols(i, k)])
            value = term if value is None else value + term
            value = value + dot(turned(trace), matrix[1, span(r), cols(i, k)])
        return value

    def finish_up(k):
        value = acc[j, :, span(k)]
        for h in halves:
            value = value + part_in[k, h].astype(F32)
        value = base[:, span(k)] + value
        total[:, span(k)] = value

        @pl.when(z > 0)
        def _():
            out_up[k] = value.astype(BF16)
            pass_up(k).start()

    def combine(k):
        swap(k).wait_recv()
        for h in halves:
            i = peer(2 * h)
            part_out[k, h] = (acc[i, :, span(k)] + pair_in[k, h].astype(F32)).astype(BF16)
        for h in halves:
            share(h, k).start()
        acc[j, :, span(k)] += pair_in[k, 0].astype(F32)

    def up(early):
        acc[...] = jnp.zeros_like(acc)

        @pl.loop(0, early)
        def _(r):
            wait_load(r)
            wait_up(r)
            for i in range(peers):
                for k in range(blocks):
                    acc[i, :, span(k)] += up_term(i, k, [r])

        @pl.loop(early, blocks)
        def _(r):
            wait_load(r)
            wait_up(r)

        late = range(early, blocks)

        def hand_over(k):
            for d in range(peers - 1, 0, -2):
                i = peer(d)
                pair_out[k, d // 2] = (acc[i, :, span(k)] + up_term(i, k, late)).astype(BF16)

        def keep(k):
            for d in range(peers - 2, -1, -2):
                i = peer(d)
                acc[i, :, span(k)] += up_term(i, k, late)

        ahead = min(AHEAD, blocks)

        @pl.loop(0, ahead)
        def _(k):
            hand_over(k)
            swap(k).start()

        @pl.loop(0, blocks)
        def _(k):
            @pl.when(k + ahead < blocks)
            def _():
                hand_over(k + ahead)
                swap(k + ahead).start()

            keep(k)
            combine(k)

        @pl.loop(0, blocks)
        def _(k):
            shares = pl.ds(0, len(halves))
            remote(part_out.at[k, shares], part_in.at[k, shares], psend, precv.at[k], {"sweep": z}).wait_recv()
            finish_up(k)

        sent(pair_out, xsend)
        sent(part_out.at[:, pl.ds(0, len(halves))], psend)

    @pl.when(z < layers - 1)
    def _():
        up(blocks // 2)

    @pl.when(z < layers - 1)
    def _():
        sent(out_down, dsend)
        if far:
            sent(gathered.at[:, pl.ds(0, len(far))], fsend)

    @pl.when(z > 0)
    def _():
        sent(out_up, usend)
        sent(gathered.at[:, pl.ds(0, len(near))], gsend)


def local(layers, peers, green, down_source, up_source):
    _one, parts, own, wide = green.shape
    sources = down_source.shape[2]
    both = parts * sources
    width = next(w for w in (256, 128) if own % w == 0)
    blocks = own // width
    groups = min(GROUPS, peers)
    vmem = pl.BlockSpec(memory_space=pltpu.VMEM)
    dma = pltpu.SemaphoreType.DMA
    result = pl.pallas_call(
        functools.partial(sweeps, layers, peers, blocks),
        out_shape=pltpu.VMEM((both, own), F32),
        in_specs=[pl.BlockSpec(memory_space=pltpu.HBM)] * 3,
        out_specs=vmem,
        scratch_shapes=[
            pltpu.VMEM((parts, own, wide), BF16),
            pltpu.VMEM((both, own), F32),
            pltpu.VMEM((both, own), F32),
            pltpu.VMEM((blocks, peers, both, width), BF16),
            pltpu.VMEM((blocks, both, width), BF16),
            pltpu.VMEM((blocks, peers // 2, both, width), BF16),
            pltpu.VMEM((blocks, peers // 2, both, width), BF16),
            pltpu.VMEM((blocks, peers // 2, both, width), BF16),
            pltpu.VMEM((blocks, peers // 2, both, width), BF16),
            pltpu.VMEM((blocks, both, width), BF16),
            pltpu.VMEM((blocks, both, width), BF16),
            pltpu.VMEM((both, own), F32),
            pltpu.VMEM((peers, both, own), F32),
            dma((2,)),
            dma((blocks, groups)),
            dma(()), dma((blocks,)),
            dma(()), dma((blocks,)),
            dma(()), dma((blocks,)),
            dma(()), dma((blocks,)),
            dma(()), dma((blocks,)),
            dma(()), dma((blocks,)),
        ],
        compiler_params=pltpu.CompilerParams(
            collective_id=0, has_side_effects=True, vmem_limit_bytes=60 * 1024 * 1024),
    )(green[0], down_source.reshape(both, own), up_source.reshape(both, own))
    return result.reshape(1, parts, sources, own)


def solution(mesh):
    in_specs = (
        P("sweep", None, "layer", None),
        P("sweep", None, None, "layer"),
        P("sweep", None, None, "layer"),
    )
    out_specs = P("sweep", None, None, "layer")
    body = functools.partial(local, mesh.shape["sweep"], mesh.shape["layer"])
    return jax.shard_map(body, mesh=mesh, in_specs=in_specs, out_specs=out_specs, check_vma=False)
```

```python
import functools

import jax
import jax.numpy as jnp
from jax import lax
from jax.experimental import pallas as pl
from jax.experimental.pallas import tpu as pltpu
from jax.sharding import PartitionSpec as P

MESH = pl.DeviceIdType.MESH
F32, BF16 = jnp.float32, jnp.bfloat16
GROUPS = 4
EARLY = 3
AHEAD = 1


def turned(trace):
    half = trace.shape[0] // 2
    return jnp.concatenate([-trace[half:], trace[:half]], axis=0)


def dot(trace, block):
    return jnp.dot(trace, block, preferred_element_type=F32)


def sweeps(layers, peers, blocks, green, down_hbm, up_hbm, total,
           matrix, down_src, up_src, gathered, incoming, pair_out, pair_in, part_out, part_in, out_down, out_up, base, acc,
           src_sem, load_sem, dsend, drecv, gsend, grecv, fsend, frecv, usend, urecv, xsend, xrecv, psend, precv):
    z, j = lax.axis_index("sweep"), lax.axis_index("layer")
    own = down_src.shape[1]
    width = own // blocks
    groups = min(GROUPS, peers)
    per = peers // groups
    odd = lax.rem(z, 2) == 1

    def span(k):
        return pl.ds(pl.multiple_of(k * width, width), width)

    def cols(i, k):
        return pl.ds(pl.multiple_of(i * own + k * width, width), width)

    def peer(d):
        i, bit = j, 1
        while bit < peers:
            if d & bit:
                i = i + bit - 2 * bit * lax.rem(j // bit, 2)
            bit *= 2
        return i

    others = range(peers - 1, 0, -1)
    far = [d for d in others if bin(d // 2).count("1") > 1]
    near = [d for d in others if d not in far]
    soon, later = [0, 1] + far, [d for d in near if d > 1]
    halves = range(peers // 2 - 1, 0, -1)

    def load(m, g):
        at = (slice(None), span(m), pl.ds(g * per * own, per * own))
        return pltpu.make_async_copy(green.at[at], matrix.at[at], load_sem.at[m, g])

    def start_loads():
        for m in range(blocks):
            for g in range(groups):
                load(m, g).start()

    def wait_load(m):
        for g in range(groups):
            load(m, g).wait()

    sources = [pltpu.make_async_copy(down_hbm, down_src, src_sem.at[0]),
               pltpu.make_async_copy(up_hbm, up_src, src_sem.at[1])]

    def remote(src, dst, send, recv, to):
        return pltpu.make_async_remote_copy(
            src_ref=src, dst_ref=dst, send_sem=send, recv_sem=recv, device_id=to, device_id_type=MESH)

    def pass_down(k):
        return remote(out_down.at[k], gathered.at[k, j], dsend, drecv.at[k], {"sweep": z + 1})

    def pass_far(k, d):
        return remote(out_down.at[k], gathered.at[k, j], fsend, frecv.at[k],
                      {"sweep": z + 1, "layer": peer(d)})

    def pass_up(k):
        return remote(out_up.at[k], incoming.at[k], usend, urecv.at[k], {"sweep": z - 1})

    def relay(k, d):
        return remote(gathered.at[k, j], gathered.at[k, j], gsend, (frecv if d == 1 else grecv).at[k],
                      {"layer": peer(d)})

    def swap(k):
        return remote(pair_out.at[k], pair_in.at[k], xsend, xrecv.at[k], {"layer": peer(1)})

    def share(h, k):
        return remote(part_out.at[k, h], part_in.at[k, h], psend, precv.at[k], {"layer": peer(2 * h)})

    barrier = pltpu.get_barrier_semaphore()

    def sent(sources_of, sem):
        remote(sources_of, sources_of, sem, sem, {"sweep": z}).wait_send()

    def greet(to):
        pl.semaphore_signal(barrier, inc=1, device_id=to, device_id_type=MESH)

    @pl.when(z > 0)
    def _():
        for d in far:
            greet({"sweep": z - 1, "layer": peer(d)})
        greet({"sweep": z - 1})
        start_loads()
        for d in others:
            greet({"layer": peer(d)})

    for copy in sources:
        copy.start()

    def take(k):
        remote(out_down.at[k], gathered.at[k, j], dsend, drecv.at[k], {"sweep": z}).wait_recv()
        for d in near:
            relay(k, d).start()

    def flip(m, g):
        load(m, g).wait()
        for i in range(g * per, (g + 1) * per):
            for k in range(blocks):
                for part in (0, 1):
                    at = (part, span(m), cols(i, k))
                    matrix[at] = matrix[at].T

    @pl.when(z > 0)
    def _():
        for g in range(groups):
            flip(0, g)

    @pl.when(z == 0)
    def _():
        pl.semaphore_wait(barrier, 1 + len(far))

    @pl.when((z > 0) & (z < layers - 1))
    def _():
        pl.semaphore_wait(barrier, peers + len(far))

    @pl.when(z == layers - 1)
    def _():
        pl.semaphore_wait(barrier, peers - 1)

    def finish_down(k, value, last):
        sum_of = up_src[:, span(k)] + value

        def go_on():
            base[:, span(k)] = sum_of
            out_down[k] = value.astype(BF16)
            for d in far:
                pass_far(k, d).start()
            pass_down(k).start()

        def turn_back():
            total[:, span(k)] = sum_of
            out_up[k] = sum_of.astype(BF16)
            pass_up(k).start()

        if last is None:
            pl.when(z < layers - 1)(go_on)
            pl.when(z == layers - 1)(turn_back)
        elif last:
            turn_back()
        else:
            go_on()

    even_last = None if layers % 2 else False
    odd_last = True if layers == 4 else None

    def wait_some(k, count, sem):
        if count:
            some = gathered.at[k, pl.ds(0, count)]
            remote(some, some, gsend, sem.at[k], {"sweep": z}).wait_recv()

    def wait_soon(k):
        wait_some(k, len(soon) - 1, frecv)

    def wait_later(k):
        wait_some(k, len(later), grecv)

    def wait_gather(k):
        wait_soon(k)
        wait_later(k)

    def down_term(m, pairs):
        value = jnp.zeros((down_src.shape[0], width), F32) if not pairs else None
        for k, ds in pairs:
            for i in (range(peers) if ds is None else map(peer, ds)):
                trace = gathered[k, i]
                term = dot(trace, matrix[0, span(m), cols(i, k)])
                value = term if value is None else value + term
                value = value + dot(turned(trace), matrix[1, span(m), cols(i, k)])
        return value

    def again():
        @pl.when(z < layers - 1)
        def _():
            start_loads()

    def wait_sources():
        for copy in sources:
            copy.wait()

    @pl.when(z == 0)
    def _():
        wait_sources()

        @pl.loop(0, blocks)
        def _(k):
            finish_down(k, down_src[:, span(k)], False)

        start_loads()

    @pl.when(z > 0)
    def _():
        @pl.loop(1, blocks)
        def _(m):
            for g in range(groups):
                flip(m, g)
                if g % 2 == 0:
                    @pl.when((z == 1) & (m == blocks // 2))
                    def _():
                        @pl.loop(g // 2 * blocks // 2, (g // 2 + 1) * blocks // 2)
                        def _(k):
                            take(k)
        wait_sources()

    @pl.when(z == 1)
    def _():
        @pl.loop(0, blocks)
        def _(k):
            wait_gather(k)

        @pl.loop(0, blocks)
        def _(m):
            finish_down(m, down_src[:, span(m)] + down_term(m, [(k, None) for k in range(blocks)]), False)

        again()

    @pl.when(odd & (z > 1))
    def _():
        early = min(EARLY, blocks)
        base[...] = down_src[...]

        @pl.loop(0, blocks)
        def _(k):
            take(k)

        @pl.loop(0, early)
        def _(k):
            wait_soon(k)
            for m in range(blocks):
                base[:, span(m)] += down_term(m, [(k, soon)])

        @pl.loop(early, blocks)
        def _(k):
            wait_soon(k)

        @pl.loop(0, blocks)
        def _(k):
            wait_later(k)

        left = [(k, later) for k in range(early)] + [(k, soon + later) for k in range(early, blocks)]

        @pl.loop(0, blocks)
        def _(m):
            finish_down(m, base[:, span(m)] + down_term(m, left), odd_last)

        again()

    @pl.when(jnp.logical_not(odd) & (z > 0))
    def _():
        base[...] = down_src[...]
        take(0)
        wait_soon(0)
        if blocks > 1:
            take(1)

        @pl.loop(0, blocks - 1)
        def _(k):
            @pl.when(k > 0)
            def _():
                wait_soon(k)

            for m in range(blocks):
                base[:, span(m)] += down_term(m, [(k, soon)])

            @pl.when(k + 2 < blocks)
            def _():
                take(k + 2)

            wait_later(k)
            for m in range(blocks):
                base[:, span(m)] += down_term(m, [(k, later)])

        last = blocks - 1
        if last:
            wait_soon(last)
        for m in range(blocks):
            base[:, span(m)] += down_term(m, [(last, soon)])
        wait_later(last)
        for m in range(blocks):
            finish_down(m, base[:, span(m)] + down_term(m, [(last, later)]), even_last)

        again()

    def wait_up(k):
        remote(out_up.at[k], incoming.at[k], usend, urecv.at[k], {"sweep": z}).wait_recv()

    def up_term(i, k, rs):
        value = None
        for r in rs:
            trace = incoming[r]
            term = dot(trace, matrix[0, span(r), cols(i, k)])
            value = term if value is None else value + term
            value = value + dot(turned(trace), matrix[1, span(r), cols(i, k)])
        return value

    def finish_up(k):
        value = acc[j, :, span(k)]
        for h in halves:
            value = value + part_in[k, h].astype(F32)
        value = base[:, span(k)] + value
        total[:, span(k)] = value

        @pl.when(z > 0)
        def _():
            out_up[k] = value.astype(BF16)
            pass_up(k).start()

    def combine(k):
        swap(k).wait_recv()
        for h in halves:
            i = peer(2 * h)
            part_out[k, h] = (acc[i, :, span(k)] + pair_in[k, h].astype(F32)).astype(BF16)
        for h in halves:
            share(h, k).start()
        acc[j, :, span(k)] += pair_in[k, 0].astype(F32)

    def up(early):
        acc[...] = jnp.zeros_like(acc)

        @pl.loop(0, early)
        def _(r):
            wait_load(r)
            wait_up(r)
            for i in range(peers):
                for k in range(blocks):
                    acc[i, :, span(k)] += up_term(i, k, [r])

        @pl.loop(early, blocks)
        def _(r):
            wait_load(r)
            wait_up(r)

        late = range(early, blocks)

        def hand_over(k):
            for d in range(peers - 1, 0, -2):
                i = peer(d)
                pair_out[k, d // 2] = (acc[i, :, span(k)] + up_term(i, k, late)).astype(BF16)

        def keep(k):
            for d in range(peers - 2, -1, -2):
                i = peer(d)
                acc[i, :, span(k)] += up_term(i, k, late)

        ahead = min(AHEAD, blocks)

        @pl.loop(0, ahead)
        def _(k):
            hand_over(k)
            swap(k).start()

        @pl.loop(0, blocks)
        def _(k):
            @pl.when(k + ahead < blocks)
            def _():
                hand_over(k + ahead)
                swap(k + ahead).start()

            keep(k)
            combine(k)

        @pl.loop(0, blocks)
        def _(k):
            shares = pl.ds(0, len(halves))
            remote(part_out.at[k, shares], part_in.at[k, shares], psend, precv.at[k], {"sweep": z}).wait_recv()
            finish_up(k)

        sent(pair_out, xsend)
        sent(part_out.at[:, pl.ds(0, len(halves))], psend)

    @pl.when(z < layers - 1)
    def _():
        up(blocks // 2)

    @pl.when(z < layers - 1)
    def _():
        sent(out_down, dsend)
        if far:
            sent(gathered.at[:, pl.ds(0, len(far))], fsend)

    @pl.when(z > 0)
    def _():
        sent(out_up, usend)
        sent(gathered.at[:, pl.ds(0, len(near))], gsend)


def local(layers, peers, green, down_source, up_source):
    _one, parts, own, wide = green.shape
    sources = down_source.shape[2]
    both = parts * sources
    width = next(w for w in (256, 128) if own % w == 0)
    blocks = own // width
    groups = min(GROUPS, peers)
    vmem = pl.BlockSpec(memory_space=pltpu.VMEM)
    dma = pltpu.SemaphoreType.DMA
    result = pl.pallas_call(
        functools.partial(sweeps, layers, peers, blocks),
        out_shape=pltpu.VMEM((both, own), F32),
        in_specs=[pl.BlockSpec(memory_space=pltpu.HBM)] * 3,
        out_specs=vmem,
        scratch_shapes=[
            pltpu.VMEM((parts, own, wide), BF16),
            pltpu.VMEM((both, own), F32),
            pltpu.VMEM((both, own), F32),
            pltpu.VMEM((blocks, peers, both, width), BF16),
            pltpu.VMEM((blocks, both, width), BF16),
            pltpu.VMEM((blocks, peers // 2, both, width), BF16),
            pltpu.VMEM((blocks, peers // 2, both, width), BF16),
            pltpu.VMEM((blocks, peers // 2, both, width), BF16),
            pltpu.VMEM((blocks, peers // 2, both, width), BF16),
            pltpu.VMEM((blocks, both, width), BF16),
            pltpu.VMEM((blocks, both, width), BF16),
            pltpu.VMEM((both, own), F32),
            pltpu.VMEM((peers, both, own), F32),
            dma((2,)),
            dma((blocks, groups)),
            dma(()), dma((blocks,)),
            dma(()), dma((blocks,)),
            dma(()), dma((blocks,)),
            dma(()), dma((blocks,)),
            dma(()), dma((blocks,)),
            dma(()), dma((blocks,)),
        ],
        compiler_params=pltpu.CompilerParams(
            collective_id=0, has_side_effects=True, vmem_limit_bytes=60 * 1024 * 1024),
    )(green[0], down_source.reshape(both, own), up_source.reshape(both, own))
    return result.reshape(1, parts, sources, own)


def solution(mesh):
    in_specs = (
        P("sweep", None, "layer", None),
        P("sweep", None, None, "layer"),
        P("sweep", None, None, "layer"),
    )
    out_specs = P("sweep", None, None, "layer")
    body = functools.partial(local, mesh.shape["sweep"], mesh.shape["layer"])
    return jax.shard_map(body, mesh=mesh, in_specs=in_specs, out_specs=out_specs, check_vma=False)
```

```python
import functools

import jax
import jax.numpy as jnp
from jax import lax
from jax.experimental import pallas as pl
from jax.experimental.pallas import tpu as pltpu
from jax.sharding import PartitionSpec as P

MESH = pl.DeviceIdType.MESH
F32, BF16 = jnp.float32, jnp.bfloat16
GROUPS = 4
EARLY = 3
AHEAD = 1


def turned(trace):
    half = trace.shape[0] // 2
    return jnp.concatenate([-trace[half:], trace[:half]], axis=0)


def dot(trace, block):
    return jnp.dot(trace, block, preferred_element_type=F32)


def sweeps(layers, peers, blocks, green, down_hbm, up_hbm, total,
           matrix, down_src, up_src, gathered, incoming, pair_out, pair_in, part_out, part_in, out_down, out_up, base, acc,
           src_sem, load_sem, dsend, drecv, gsend, grecv, fsend, frecv, usend, urecv, xsend, xrecv, psend, precv):
    z, j = lax.axis_index("sweep"), lax.axis_index("layer")
    own = down_src.shape[1]
    width = own // blocks
    groups = min(GROUPS, peers)
    per = peers // groups
    odd = lax.rem(z, 2) == 1

    def span(k):
        return pl.ds(pl.multiple_of(k * width, width), width)

    def cols(i, k):
        return pl.ds(pl.multiple_of(i * own + k * width, width), width)

    def peer(d):
        i, bit = j, 1
        while bit < peers:
            if d & bit:
                i = i + bit - 2 * bit * lax.rem(j // bit, 2)
            bit *= 2
        return i

    others = range(peers - 1, 0, -1)
    far = [d for d in others if bin(d // 2).count("1") > 1]
    near = [d for d in others if d not in far]
    soon, later = [0, 1] + far, [d for d in near if d > 1]
    halves = range(peers // 2 - 1, 0, -1)

    def load(m, g):
        at = (slice(None), span(m), pl.ds(g * per * own, per * own))
        return pltpu.make_async_copy(green.at[at], matrix.at[at], load_sem.at[m, g])

    def start_loads():
        for m in range(blocks):
            for g in range(groups):
                load(m, g).start()

    def wait_load(m):
        for g in range(groups):
            load(m, g).wait()

    sources = [pltpu.make_async_copy(down_hbm, down_src, src_sem.at[0]),
               pltpu.make_async_copy(up_hbm, up_src, src_sem.at[1])]

    def remote(src, dst, send, recv, to):
        return pltpu.make_async_remote_copy(
            src_ref=src, dst_ref=dst, send_sem=send, recv_sem=recv, device_id=to, device_id_type=MESH)

    def pass_down(k):
        return remote(out_down.at[k], gathered.at[k, j], dsend, drecv.at[k], {"sweep": z + 1})

    def pass_far(k, d):
        return remote(out_down.at[k], gathered.at[k, j], fsend, frecv.at[k],
                      {"sweep": z + 1, "layer": peer(d)})

    def pass_up(k):
        return remote(out_up.at[k], incoming.at[k], usend, urecv.at[k], {"sweep": z - 1})

    def relay(k, d):
        return remote(gathered.at[k, j], gathered.at[k, j], gsend, (frecv if d == 1 else grecv).at[k],
                      {"layer": peer(d)})

    def swap(k):
        return remote(pair_out.at[k], pair_in.at[k], xsend, xrecv.at[k], {"layer": peer(1)})

    def share(h, k):
        return remote(part_out.at[k, h], part_in.at[k, h], psend, precv.at[k], {"layer": peer(2 * h)})

    barrier = pltpu.get_barrier_semaphore()

    def sent(sources_of, sem):
        remote(sources_of, sources_of, sem, sem, {"sweep": z}).wait_send()

    def greet(to):
        pl.semaphore_signal(barrier, inc=1, device_id=to, device_id_type=MESH)

    @pl.when(z > 0)
    def _():
        for d in far:
            greet({"sweep": z - 1, "layer": peer(d)})
        greet({"sweep": z - 1})
        start_loads()
        for d in others:
            greet({"layer": peer(d)})

    for copy in sources:
        copy.start()

    def take(k):
        remote(out_down.at[k], gathered.at[k, j], dsend, drecv.at[k], {"sweep": z}).wait_recv()
        for d in near:
            relay(k, d).start()

    def flip(m, g):
        load(m, g).wait()
        for i in range(g * per, (g + 1) * per):
            for k in range(blocks):
                for part in (0, 1):
                    at = (part, span(m), cols(i, k))
                    matrix[at] = matrix[at].T

    @pl.when(z > 0)
    def _():
        for g in range(groups):
            flip(0, g)

    @pl.when(z == 0)
    def _():
        pl.semaphore_wait(barrier, 1 + len(far))

    @pl.when((z > 0) & (z < layers - 1))
    def _():
        pl.semaphore_wait(barrier, peers + len(far))

    @pl.when(z == layers - 1)
    def _():
        pl.semaphore_wait(barrier, peers - 1)

    def finish_down(k, value, last):
        sum_of = up_src[:, span(k)] + value

        def go_on():
            base[:, span(k)] = sum_of
            out_down[k] = value.astype(BF16)
            for d in far:
                pass_far(k, d).start()
            pass_down(k).start()

        def turn_back():
            total[:, span(k)] = sum_of
            out_up[k] = sum_of.astype(BF16)
            pass_up(k).start()

        if last is None:
            pl.when(z < layers - 1)(go_on)
            pl.when(z == layers - 1)(turn_back)
        elif last:
            turn_back()
        else:
            go_on()

    even_last = None if layers % 2 else False
    odd_last = True if layers == 4 else None

    def wait_some(k, count, sem):
        if count:
            some = gathered.at[k, pl.ds(0, count)]
            remote(some, some, gsend, sem.at[k], {"sweep": z}).wait_recv()

    def wait_soon(k):
        wait_some(k, len(soon) - 1, frecv)

    def wait_later(k):
        wait_some(k, len(later), grecv)

    def wait_gather(k):
        wait_soon(k)
        wait_later(k)

    def down_term(m, pairs):
        value = jnp.zeros((down_src.shape[0], width), F32) if not pairs else None
        for k, ds in pairs:
            for i in (range(peers) if ds is None else map(peer, ds)):
                trace = gathered[k, i]
                term = dot(trace, matrix[0, span(m), cols(i, k)])
                value = term if value is None else value + term
                value = value + dot(turned(trace), matrix[1, span(m), cols(i, k)])
        return value

    def again():
        @pl.when(z < layers - 1)
        def _():
            start_loads()

    def wait_sources():
        for copy in sources:
            copy.wait()

    @pl.when(z == 0)
    def _():
        wait_sources()

        @pl.loop(0, blocks)
        def _(k):
            finish_down(k, down_src[:, span(k)], False)

        start_loads()

    @pl.when(z > 0)
    def _():
        @pl.loop(1, blocks)
        def _(m):
            for g in range(groups):
                flip(m, g)
                if g % 2 == 0:
                    @pl.when((z == 1) & (m == blocks // 2))
                    def _():
                        @pl.loop(g // 2 * blocks // 2, (g // 2 + 1) * blocks // 2)
                        def _(k):
                            take(k)
        wait_sources()

    @pl.when(z == 1)
    def _():
        @pl.loop(0, blocks)
        def _(k):
            wait_gather(k)

        @pl.loop(0, blocks)
        def _(m):
            finish_down(m, down_src[:, span(m)] + down_term(m, [(k, None) for k in range(blocks)]), False)

        again()

    @pl.when(odd & (z > 1))
    def _():
        early = min(EARLY, blocks)
        base[...] = down_src[...]

        @pl.loop(0, blocks)
        def _(k):
            take(k)

        @pl.loop(0, early)
        def _(k):
            wait_soon(k)
            for m in range(blocks):
                base[:, span(m)] += down_term(m, [(k, soon)])

        @pl.loop(early, blocks)
        def _(k):
            wait_soon(k)

        @pl.loop(0, blocks)
        def _(k):
            wait_later(k)

        left = [(k, later) for k in range(early)] + [(k, soon + later) for k in range(early, blocks)]

        @pl.loop(0, blocks)
        def _(m):
            finish_down(m, base[:, span(m)] + down_term(m, left), odd_last)

        again()

    @pl.when(jnp.logical_not(odd) & (z > 0))
    def _():
        base[...] = down_src[...]
        take(0)
        wait_soon(0)
        if blocks > 1:
            take(1)

        @pl.loop(0, blocks - 1)
        def _(k):
            @pl.when(k > 0)
            def _():
                wait_soon(k)

            for m in range(blocks):
                base[:, span(m)] += down_term(m, [(k, soon)])

            @pl.when(k + 2 < blocks)
            def _():
                take(k + 2)

            wait_later(k)
            for m in range(blocks):
                base[:, span(m)] += down_term(m, [(k, later)])

        last = blocks - 1
        if last:
            wait_soon(last)
        for m in range(blocks):
            base[:, span(m)] += down_term(m, [(last, soon)])
        wait_later(last)
        for m in range(blocks):
            finish_down(m, base[:, span(m)] + down_term(m, [(last, later)]), even_last)

        again()

    def wait_up(k):
        remote(out_up.at[k], incoming.at[k], usend, urecv.at[k], {"sweep": z}).wait_recv()

    def up_term(i, k, rs):
        value = None
        for r in rs:
            trace = incoming[r]
            term = dot(trace, matrix[0, span(r), cols(i, k)])
            value = term if value is None else value + term
            value = value + dot(turned(trace), matrix[1, span(r), cols(i, k)])
        return value

    def finish_up(k):
        value = acc[j, :, span(k)]
        for h in halves:
            value = value + part_in[k, h].astype(F32)
        value = base[:, span(k)] + value
        total[:, span(k)] = value

        @pl.when(z > 0)
        def _():
            out_up[k] = value.astype(BF16)
            pass_up(k).start()

    def combine(k):
        swap(k).wait_recv()
        for h in halves:
            i = peer(2 * h)
            part_out[k, h] = (acc[i, :, span(k)] + pair_in[k, h].astype(F32)).astype(BF16)
            share(h, k).start()
        acc[j, :, span(k)] += pair_in[k, 0].astype(F32)

    def up(early):
        acc[...] = jnp.zeros_like(acc)

        @pl.loop(0, early)
        def _(r):
            wait_load(r)
            wait_up(r)
            for i in range(peers):
                for k in range(blocks):
                    acc[i, :, span(k)] += up_term(i, k, [r])

        @pl.loop(early, blocks)
        def _(r):
            wait_load(r)
            wait_up(r)

        late = range(early, blocks)

        def hand_over(k):
            for d in range(peers - 1, 0, -2):
                i = peer(d)
                pair_out[k, d // 2] = (acc[i, :, span(k)] + up_term(i, k, late)).astype(BF16)

        def keep(k):
            for d in range(peers - 2, -1, -2):
                i = peer(d)
                acc[i, :, span(k)] += up_term(i, k, late)

        ahead = min(AHEAD, blocks)

        @pl.loop(0, ahead)
        def _(k):
            hand_over(k)
            swap(k).start()

        @pl.loop(0, blocks)
        def _(k):
            @pl.when(k + ahead < blocks)
            def _():
                hand_over(k + ahead)
                swap(k + ahead).start()

            keep(k)
            combine(k)

        @pl.loop(0, blocks)
        def _(k):
            shares = pl.ds(0, len(halves))
            remote(part_out.at[k, shares], part_in.at[k, shares], psend, precv.at[k], {"sweep": z}).wait_recv()
            finish_up(k)

        sent(pair_out, xsend)
        sent(part_out.at[:, pl.ds(0, len(halves))], psend)

    @pl.when(z < layers - 1)
    def _():
        up(blocks // 2)

    @pl.when(z < layers - 1)
    def _():
        sent(out_down, dsend)
        if far:
            sent(gathered.at[:, pl.ds(0, len(far))], fsend)

    @pl.when(z > 0)
    def _():
        sent(out_up, usend)
        sent(gathered.at[:, pl.ds(0, len(near))], gsend)


def local(layers, peers, green, down_source, up_source):
    _one, parts, own, wide = green.shape
    sources = down_source.shape[2]
    both = parts * sources
    width = next(w for w in (256, 128) if own % w == 0)
    blocks = own // width
    groups = min(GROUPS, peers)
    vmem = pl.BlockSpec(memory_space=pltpu.VMEM)
    dma = pltpu.SemaphoreType.DMA
    result = pl.pallas_call(
        functools.partial(sweeps, layers, peers, blocks),
        out_shape=pltpu.VMEM((both, own), F32),
        in_specs=[pl.BlockSpec(memory_space=pltpu.HBM)] * 3,
        out_specs=vmem,
        scratch_shapes=[
            pltpu.VMEM((parts, own, wide), BF16),
            pltpu.VMEM((both, own), F32),
            pltpu.VMEM((both, own), F32),
            pltpu.VMEM((blocks, peers, both, width), BF16),
            pltpu.VMEM((blocks, both, width), BF16),
            pltpu.VMEM((blocks, peers // 2, both, width), BF16),
            pltpu.VMEM((blocks, peers // 2, both, width), BF16),
            pltpu.VMEM((blocks, peers // 2, both, width), BF16),
            pltpu.VMEM((blocks, peers // 2, both, width), BF16),
            pltpu.VMEM((blocks, both, width), BF16),
            pltpu.VMEM((blocks, both, width), BF16),
            pltpu.VMEM((both, own), F32),
            pltpu.VMEM((peers, both, own), F32),
            dma((2,)),
            dma((blocks, groups)),
            dma(()), dma((blocks,)),
            dma(()), dma((blocks,)),
            dma(()), dma((blocks,)),
            dma(()), dma((blocks,)),
            dma(()), dma((blocks,)),
            dma(()), dma((blocks,)),
        ],
        compiler_params=pltpu.CompilerParams(
            collective_id=0, has_side_effects=True, vmem_limit_bytes=60 * 1024 * 1024),
    )(green[0], down_source.reshape(both, own), up_source.reshape(both, own))
    return result.reshape(1, parts, sources, own)


def solution(mesh):
    in_specs = (
        P("sweep", None, "layer", None),
        P("sweep", None, None, "layer"),
        P("sweep", None, None, "layer"),
    )
    out_specs = P("sweep", None, None, "layer")
    body = functools.partial(local, mesh.shape["sweep"], mesh.shape["layer"])
    return jax.shard_map(body, mesh=mesh, in_specs=in_specs, out_specs=out_specs, check_vma=False)
```
